256 devices in a mesh: mem: 16 (over z, core), space: 16 (over x, y).
Axes of the slice: x: 4, y: 4, z: 8, core: 2. Of those that a mesh axis runs over, the one named last changes fastest.
Arguments:
- dp_fore: float32 [1024, 64, 16, 128], P('space', 'mem'), may hold values from 0.5 to 2
- hum_fore: float32 [1024, 64, 16, 128], P('space', 'mem'), may hold values from 0 to 0.2
- area: float32 [1024, 128], P('space'), may hold values from 0.2 to 6, as said below
- region: int32 [1024], P('space'), may hold values from 0 to 63
- weights: float32 [64, 64, 64], replicated, may hold values from 0 to 1.5, as said below
- target: float32 [64], P('mem'), may hold values from 1 to 3
Outputs:
- dp_out: float32 [1024, 64, 16, 128], P('space', 'mem')
- hum_out: float32 [1024, 64, 16, 128], P('space', 'mem')
The draws below stay inside these ranges and needn't reach their ends.
Inputs may be any that keep to these rules, and one draw needn't show every extreme that they name: Every column's area weight is positive. `weights`: all entries are non-negative; diagonal entries are 0.5 or more and off-diagonal ones 0.05 or less.
All inputs are finite; a program needn't handle non-finite values.
Results may differ from the reference program's by a relative error of at most 0.000086.
Values sent between devices are 32-bit elements; how exact they have to be, the bound alone decides.
No kernel may reach another device: no remote copies, remote signals or barrier semaphores. Data moves between devices by JAX's collectives and lax.ppermute only.
A program may use at most 64 MiB of HBM per device.

```python
import math
import jax
import jax.numpy as jnp
from jax import lax

LEV = 16
BLK = 128
REGIONS = 64
K = 64
NCOL = 131072
NBLK = 1024


def draw_area(key, part):
    ramp = 1.0 + 2.0 * jnp.arange(NCOL, dtype=jnp.float32) / (NCOL - 1)
    rough = jnp.exp(jax.random.uniform(key, (NCOL,), jnp.float32, jnp.log(0.5), jnp.log(2.0)))
    return (ramp * rough).reshape(NBLK, BLK)


def draw_weights(key, part):
    first = jax.random.fold_in(key, 11)
    second = jax.random.fold_in(key, 23)
    eye = jnp.eye(K, dtype=jnp.float32)[None, :, :]
    diag = jax.random.uniform(first, (REGIONS, K, 1), jnp.float32, 0.8, 1.2)
    off = jax.random.uniform(second, (REGIONS, K, K), jnp.float32, 0.0, 0.03)
    return eye * diag + (1.0 - eye) * off


def place_ends(drawn, key, least, high):
    spot = [jax.random.randint(jax.random.fold_in(key, axis), (), 0, length) for axis, length in enumerate(drawn.shape)]
    longest = drawn.shape.index(max(drawn.shape))
    next_to = spot[:longest] + [(spot[longest] + 1) % drawn.shape[longest]] + spot[longest + 1:]
    return drawn.at[tuple(spot)].set(least).at[tuple(next_to)].set(high)


def block_scale(rng, shape, split, low, high):
    gain = 1.0
    for dim, blocks in split:
        steps = jax.random.uniform(jax.random.fold_in(jax.random.fold_in(rng, 6), dim), (blocks,), jnp.float32, low / len(split), high / len(split))
        gain = gain * jnp.repeat(jnp.exp(steps), shape[dim] // blocks).reshape((-1,) + (1,) * (len(shape) - 1 - dim))
    return gain


def setup_inputs(seed: int = 0) -> dict:
    arg_keys = jax.random.split(jax.random.key(seed), 7)
    dp_fore = jnp.clip(jnp.exp(math.log(2.0) - 1.3862944 * jax.random.uniform(arg_keys[0], (NBLK, K, LEV, BLK), jnp.float32) ** block_scale(arg_keys[0], (NBLK, K, LEV, BLK), ((0, 16), (1, 16)), -0.2, 0.2)), 0.5, 2.0)
    hum_fore = jnp.clip(0.2 * jax.random.uniform(arg_keys[1], (NBLK, K, LEV, BLK), jnp.float32) ** block_scale(arg_keys[1], (NBLK, K, LEV, BLK), ((0, 16), (1, 16)), -0.2, 0.2), 0.0, 0.2)
    area = draw_area(jax.random.fold_in(arg_keys[6], 71), 0)
    region = place_ends(jax.random.randint(arg_keys[3], (NBLK,), 0, REGIONS), jax.random.fold_in(arg_keys[3], 1), 0, REGIONS - 1).astype(jnp.int32)
    weights = draw_weights(jax.random.fold_in(arg_keys[6], 71), 0)
    target = jnp.clip(1.0 + 2.0 * jax.random.uniform(arg_keys[5], (K,), jnp.float32) ** block_scale(arg_keys[5], (K,), ((0, 16),), -0.2, 0.2), 1.0, 3.0)
    return {"dp_fore": dp_fore, "hum_fore": hum_fore, "area": area, "region": region, "weights": weights, "target": target}


def reference(dp_fore, hum_fore, area, region, weights, target):
    nblocks, members, levels, width = dp_fore.shape
    tables = jnp.swapaxes(jnp.take(weights, region, axis=0), 1, 2)

    def mixing(field):
        flat = field.reshape(nblocks, members, levels * width)
        mixed = jnp.einsum("bkj,bjx->bkx", tables, flat, precision=lax.Precision.HIGHEST)
        return mixed.reshape(nblocks, members, levels, width)

    dp_mix = mixing(dp_fore)
    hum_mix = mixing(hum_fore)
    mass = jnp.sum(area[:, None, None, :] * dp_mix * (1.0 - hum_mix), axis=(0, 2, 3)) / (nblocks * width * levels)
    factor = target / mass
    return dp_mix * factor[None, :, None, None], hum_mix
```

```python
import functools

import jax
import jax.numpy as jnp
from jax import lax
from jax.experimental import pallas as pl
from jax.experimental.pallas import tpu as pltpu
from jax.sharding import PartitionSpec as P


HBM = pl.BlockSpec(memory_space=pltpu.HBM)
SMEM = pl.BlockSpec(memory_space=pltpu.SMEM)
VMEM = pl.BlockSpec(memory_space=pltpu.VMEM)
PARAMS = pltpu.CompilerParams(vmem_limit_bytes=60 * 1024 * 1024)


def shifts_of(chips):
    half = chips // 2
    steps = [half] if chips > 1 else []
    for d in range(half - 1, 0, -1):
        steps += [d, -d]
    moves = [(d, f) for d in steps for f in (0, 1)]
    return moves + [(0, 1), (0, 0)]


def pairs_of(chips, d, f):
    return [(2 * z + c, 2 * ((z + d) % chips) + (c ^ f)) for z in range(chips) for c in range(2)]


def other(me, chips, d, f):
    z, c = me // 2, me % 2
    return 2 * lax.rem(z + (d + chips), chips) + (c if f == 0 else 1 - c)


def cut_kernel(moves, chips, share, x_ref, *refs):
    count = len(moves) - 1
    outs, (buf, sem_in, sem_out) = refs[:count], refs[count:]
    me = lax.axis_index("mem")
    loads, stores = [], []
    for i, (d, f) in enumerate(moves[:-1]):
        to = other(me, chips, d, f)
        loads.append(pltpu.make_async_copy(x_ref.at[pl.ds(to * share, share)], buf.at[i], sem_in.at[i]))
        stores.append(pltpu.make_async_copy(buf.at[i], outs[i], sem_out.at[i]))
    for copy in loads:
        copy.start()
    for load, store in zip(loads, stores):
        load.wait()
        store.start()
    for copy in stores:
        copy.wait()


def cut(x, moves, chips, share):
    piece = jax.ShapeDtypeStruct((share, *x.shape[1:]), x.dtype)
    count = len(moves) - 1
    dma = pltpu.SemaphoreType.DMA
    return pl.pallas_call(
        functools.partial(cut_kernel, moves, chips, share),
        in_specs=[HBM],
        out_specs=[HBM] * count,
        out_shape=[piece] * count,
        scratch_shapes=[pltpu.VMEM((count, *piece.shape), x.dtype), dma((count,)), dma((count,))],
        compiler_params=PARAMS,
        name="cut",
    )(x)


def mix_kernel(moves, chips, share, levels, second, *refs):
    count = len(moves)
    region_ref, weights_ref, x_ref = refs[:3]
    pieces = refs[3 : 2 + count]
    at = 2 + count
    if second:
        area_ref = refs[at]
        firsts = refs[at + 1 : at + 1 + count]
        at += 1 + count
    outs = refs[at : at + count]
    at += count
    if second:
        mass_ref = refs[at]
        at += 1
    if second:
        x_buf, y_buf, f_buf, w_buf, sem_w, sem_in, sem_f, sem_out = refs[at:]
    else:
        x_buf, y_buf, w_buf, sem_w, sem_in, sem_out = refs[at:]
    me = lax.axis_index("mem")
    rows = x_ref.shape[1]
    members = w_buf.shape[1]
    width = x_ref.shape[2]

    copies = []
    for b in range(share):
        table = region_ref[me * share + b]
        copies.append(pltpu.make_async_copy(weights_ref.at[table], w_buf.at[b], sem_w.at[b]))
    for i, (d, f) in enumerate(moves):
        source = other(me, chips, -d, f)
        spot = pl.ds(pl.multiple_of(source * rows, rows), rows)
        held = x_ref.at[pl.ds(me * share, share)] if i == count - 1 else pieces[i]
        copies.append(pltpu.make_async_copy(held, x_buf.at[:, spot], sem_in.at[i]))
    if second:
        for i, (d, f) in enumerate(moves):
            target = other(me, chips, d, f)
            spot = pl.ds(pl.multiple_of(target * rows, rows), rows)
            copies.append(pltpu.make_async_copy(firsts[i], f_buf.at[:, spot], sem_f.at[i]))
    for copy in copies:
        copy.start()
    for copy in copies:
        copy.wait()

    step = 4
    if second:
        total = jnp.zeros((members, width), jnp.float32)
    for b in range(share):
        table = w_buf[b]
        for first in range(0, levels, step):
            x = jnp.concatenate(
                [x_buf[b, pl.ds(first + l, members, stride=levels), :] for l in range(step)], axis=1
            )
            y = lax.dot_general(
                table,
                x,
                (((0,), (0,)), ((), ())),
                precision=lax.Precision.HIGHEST,
                preferred_element_type=jnp.float32,
            )
            for l in range(step):
                part = y[:, l * width : (l + 1) * width]
                y_buf[b, pl.ds(first + l, members, stride=levels), :] = part
                if second:
                    mixed = f_buf[b, pl.ds(first + l, members, stride=levels), :]
                    total += area_ref[b] * mixed * (1.0 - part)
    if second:
        mass_ref[...] = total

    copies = []
    for i, (d, f) in enumerate(moves):
        target = other(me, chips, d, f)
        spot = pl.ds(pl.multiple_of(target * rows, rows), rows)
        copies.append(pltpu.make_async_copy(y_buf.at[:, spot], outs[i], sem_out.at[i]))
    for copy in copies:
        copy.start()
    for copy in copies:
        copy.wait()


def mix(region, weights, x, pieces, moves, chips, share, levels, area=None, firsts=None):
    second = area is not None
    count = len(moves)
    rows, width = x.shape[1:]
    members = weights.shape[1]
    piece = jax.ShapeDtypeStruct((share, rows, width), jnp.float32)
    whole = pltpu.VMEM((share, members * levels, width), jnp.float32)
    dma = pltpu.SemaphoreType.DMA
    in_specs = [SMEM, HBM, HBM] + [HBM] * (count - 1)
    args = [region, weights, x, *pieces]
    out_shape = [piece] * count
    out_specs = [HBM] * count
    scratch = [whole, whole] + [whole] * second
    scratch += [pltpu.VMEM((share, members, members), jnp.float32), dma((share,)), dma((count,))]
    scratch += [dma((count,))] * second + [dma((count,))]
    if second:
        in_specs += [VMEM] + [HBM] * count
        args += [area, *firsts]
        out_shape.append(jax.ShapeDtypeStruct((members, width), jnp.float32))
        out_specs.append(VMEM)
    return pl.pallas_call(
        functools.partial(mix_kernel, moves, chips, share, levels, second),
        in_specs=in_specs,
        out_specs=out_specs,
        out_shape=out_shape,
        scratch_shapes=scratch,
        compiler_params=PARAMS,
        name="mix2" if second else "mix1",
    )(*args)


def join_kernel(moves, chips, share, levels, scaled, *refs):
    count = len(moves)
    me = lax.axis_index("mem")
    if scaled:
        factor_ref, refs = refs[0], refs[1:]
    pieces, (out_ref, buf, sem_in, sem_out) = refs[:count], refs[count:]
    loads, stores = [], []
    for i, (d, f) in enumerate(moves):
        source = other(me, chips, -d, f)
        loads.append(pltpu.make_async_copy(pieces[i], buf.at[i], sem_in.at[i]))
        stores.append(
            pltpu.make_async_copy(buf.at[i], out_ref.at[pl.ds(source * share, share)], sem_out.at[i])
        )
    for copy in loads:
        copy.start()
    for i in range(count):
        loads[i].wait()
        if scaled:
            for member in range(buf.shape[2] // levels):
                spot = pl.ds(member * levels, levels)
                buf[i, :, spot, :] = buf[i, :, spot, :] * factor_ref[member]
        stores[i].start()
    for copy in stores:
        copy.wait()


def join(pieces, moves, chips, share, levels, factor=None):
    count = len(moves)
    shape = (count * share, *pieces[0].shape[1:])
    dma = pltpu.SemaphoreType.DMA
    scaled = factor is not None
    return pl.pallas_call(
        functools.partial(join_kernel, moves, chips, share, levels, scaled),
        in_specs=[SMEM] * scaled + [HBM] * count,
        out_specs=HBM,
        out_shape=jax.ShapeDtypeStruct(shape, jnp.float32),
        scratch_shapes=[pltpu.VMEM((count, *pieces[0].shape), jnp.float32), dma((count,)), dma((count,))],
        compiler_params=PARAMS,
        name="join_scaled" if scaled else "join",
    )(*([factor] if scaled else []), *pieces)


def per_device(dp_fore, hum_fore, area, region, weights, target):
    nblocks, mine, levels, width = dp_fore.shape
    groups = lax.axis_size("mem")
    chips = groups // 2
    share = nblocks // groups
    me = lax.axis_index("mem")
    count_all = nblocks * width * lax.axis_size("space") * levels
    moves = shifts_of(chips)

    def send(pieces, name):
        with jax.named_scope(name):
            return [
                lax.ppermute(piece, "mem", pairs_of(chips, d, f))
                for piece, (d, f) in zip(pieces, moves[:-1])
            ]

    dp = dp_fore.reshape(nblocks, mine * levels, width)
    hum = hum_fore.reshape(nblocks, mine * levels, width)
    own_area = lax.dynamic_slice_in_dim(area, me * share, share)

    dp_in = send(cut(dp, moves, chips, share), "dp_in")
    hum_in = send(cut(hum, moves, chips, share), "hum_in")
    dp_mixed = mix(region, weights, dp, dp_in, moves, chips, share, levels)
    dp_back = send(dp_mixed[:-1], "dp_back") + [dp_mixed[-1]]
    *hum_mixed, partial = mix(
        region, weights, hum, hum_in, moves, chips, share, levels, own_area, dp_mixed
    )
    with jax.named_scope("mass"):
        parts = jnp.sum(partial, axis=1).reshape(groups, mine)
        local = lax.all_to_all(parts, "mem", 0, 0, tiled=True).sum(axis=0)
        spread = jnp.broadcast_to(local[None], (lax.axis_size("space"), mine))
        totals = lax.all_to_all(spread, "space", 0, 0, tiled=True).sum(axis=0)
        factor = target / (totals / count_all)
    hum_back = send(hum_mixed[:-1], "hum_back") + [hum_mixed[-1]]
    dp_out = join(dp_back, moves, chips, share, levels, factor)
    hum_out = join(hum_back, moves, chips, share, levels)
    shape = (nblocks, mine, levels, width)
    return dp_out.reshape(shape), hum_out.reshape(shape)


def solution(mesh):
    return jax.shard_map(
        per_device,
        mesh=mesh,
        in_specs=(
            P("space", "mem", None, None),
            P("space", "mem", None, None),
            P("space", None),
            P("space"),
            P(),
            P("mem"),
        ),
        out_specs=(P("space", "mem", None, None), P("space", "mem", None, None)),
        check_vma=False,
    )
```

```python
import functools

import jax
import jax.numpy as jnp
from jax import lax
from jax.experimental import pallas as pl
from jax.experimental.pallas import tpu as pltpu
from jax.sharding import PartitionSpec as P


HBM = pl.BlockSpec(memory_space=pltpu.HBM)
SMEM = pl.BlockSpec(memory_space=pltpu.SMEM)
VMEM = pl.BlockSpec(memory_space=pltpu.VMEM)
DMA = pltpu.SemaphoreType.DMA
PARAMS = pltpu.CompilerParams(vmem_limit_bytes=60 * 1024 * 1024)


def steps_of(chips):
    half = chips // 2
    steps = [half]
    for d in range(half - 1, 0, -1):
        steps += [d, -d]
    return steps


def device_at(me, chips, d, f):
    z, c = me // 2, me % 2
    return 2 * lax.rem(z + (d + chips), chips) + (c if f == 0 else 1 - c)


def sources(me, chips, share, refs):
    if len(refs) == 1:
        return [(s, refs[0].at[pl.ds(s * share, share)]) for s in range(2 * chips)]
    own, swapped, *pieces = refs
    found = []
    for piece, d in zip(pieces, steps_of(chips)):
        for f in (0, 1):
            found.append((device_at(me, chips, -d, f), piece.at[pl.ds(f * share, share)]))
    found.append((device_at(me, chips, 0, 1), swapped.at[pl.ds((me // 2) * share, share)]))
    found.append((me, own.at[pl.ds(me * share, share)]))
    return found


def run(copies):
    for copy in copies:
        copy.start()
    for copy in copies:
        copy.wait()


def relay(loads, stores):
    for copy in loads:
        copy.start()
    for load, store in zip(loads, stores):
        load.wait()
        store.start()
    for copy in stores:
        copy.wait()


def cut_kernel(chips, share, x_ref, out_ref, buf, sem_in, sem_out):
    flip = 1 - lax.axis_index("mem") % 2
    loads, stores = [], []
    for z in range(chips):
        spot = pl.ds((2 * z + flip) * share, share)
        loads.append(pltpu.make_async_copy(x_ref.at[spot], buf.at[z], sem_in.at[z]))
        stores.append(pltpu.make_async_copy(buf.at[z], out_ref.at[pl.ds(z * share, share)], sem_out.at[z]))
    relay(loads, stores)


def cut(x, chips, share):
    tail = x.shape[1:]
    return pl.pallas_call(
        functools.partial(cut_kernel, chips, share),
        in_specs=[HBM],
        out_specs=HBM,
        out_shape=jax.ShapeDtypeStruct((chips * share, *tail), x.dtype),
        scratch_shapes=[pltpu.VMEM((chips, share, *tail), x.dtype), DMA((chips,)), DMA((chips,))],
        compiler_params=PARAMS,
        name="cut",
    )(x)


def pack_kernel(chips, share, x_ref, swapped_ref, *refs):
    count = chips - 1
    outs, (buf, sem_in, sem_other, sem_out) = refs[:count], refs[count:]
    me = lax.axis_index("mem")
    loads, others, stores = [], [], []
    for i, d in enumerate(steps_of(chips)):
        to = device_at(me, chips, d, 0)
        own, rest = pl.ds(to * share, share), pl.ds((to // 2) * share, share)
        loads.append(pltpu.make_async_copy(x_ref.at[own], buf.at[i, pl.ds(0, share)], sem_in.at[i]))
        others.append(
            pltpu.make_async_copy(swapped_ref.at[rest], buf.at[i, pl.ds(share, share)], sem_other.at[i])
        )
        stores.append(pltpu.make_async_copy(buf.at[i], outs[i], sem_out.at[i]))
    for load, rest in zip(loads, others):
        load.start()
        rest.start()
    for load, rest, store in zip(loads, others, stores):
        load.wait()
        rest.wait()
        store.start()
    for copy in stores:
        copy.wait()


def pack(x, swapped, chips, share):
    piece = (2 * share, *x.shape[1:])
    count = chips - 1
    return pl.pallas_call(
        functools.partial(pack_kernel, chips, share),
        in_specs=[HBM, HBM],
        out_specs=[HBM] * count,
        out_shape=[jax.ShapeDtypeStruct(piece, x.dtype)] * count,
        scratch_shapes=[pltpu.VMEM((count, *piece), x.dtype), DMA((count,)), DMA((count,)), DMA((count,))],
        compiler_params=PARAMS,
        name="pack",
    )(x, swapped)


def mix_kernel(chips, share, levels, size, second, *refs):
    count = 2 * chips
    region_ref, weights_ref = refs[:2]
    held, refs = refs[2 : 2 + size], refs[2 + size :]
    if second:
        area_ref, first_ref, *refs = refs
    out_ref, cut_ref, *refs = refs
    if second:
        mass_ref, f_buf, sem_f, *refs = refs
    x_buf, y_buf, w_buf, sem_w, sem_in, sem_out, sem_cut = refs
    me = lax.axis_index("mem")
    flip = 1 - me % 2
    rows = out_ref.shape[1]
    width = out_ref.shape[2]
    members = w_buf.shape[1]

    def lines(place):
        return pl.ds(place * rows if isinstance(place, int) else pl.multiple_of(place * rows, rows), rows)

    copies = []
    for b in range(share):
        table = region_ref[me * share + b]
        copies.append(pltpu.make_async_copy(weights_ref.at[table], w_buf.at[b], sem_w.at[b]))
    for i, (place, blocks) in enumerate(sources(me, chips, share, held)):
        copies.append(pltpu.make_async_copy(blocks, x_buf.at[:, lines(place)], sem_in.at[i]))
    if second:
        for place in range(count):
            blocks = first_ref.at[pl.ds(place * share, share)]
            copies.append(pltpu.make_async_copy(blocks, f_buf.at[:, lines(place)], sem_f.at[place]))
    run(copies)

    step = 4
    if second:
        total = jnp.zeros((members, width), jnp.float32)
    for b in range(share):
        table = w_buf[b]
        for first in range(0, levels, step):
            x = jnp.concatenate(
                [x_buf[b, pl.ds(first + l, members, stride=levels), :] for l in range(step)], axis=1
            )
            y = lax.dot_general(
                table,
                x,
                (((0,), (0,)), ((), ())),
                precision=lax.Precision.HIGHEST,
                preferred_element_type=jnp.float32,
            )
            for l in range(step):
                part = y[:, l * width : (l + 1) * width]
                y_buf[b, pl.ds(first + l, members, stride=levels), :] = part
                if second:
                    mixed = f_buf[b, pl.ds(first + l, members, stride=levels), :]
                    total += area_ref[b] * mixed * (1.0 - part)
    if second:
        mass_ref[...] = total

    copies = []
    for z in range(chips):
        spot = pl.ds(z * share, share)
        copies.append(pltpu.make_async_copy(y_buf.at[:, lines(2 * z + flip)], cut_ref.at[spot], sem_cut.at[z]))
    for place in range(count):
        spot = pl.ds(place * share, share)
        copies.append(pltpu.make_async_copy(y_buf.at[:, lines(place)], out_ref.at[spot], sem_out.at[place]))
    run(copies)


def mix(region, weights, held, chips, share, levels, area=None, first=None):
    second = area is not None
    rows, width = held[0].shape[1:]
    members = weights.shape[1]
    count = 2 * chips
    whole = pltpu.VMEM((share, members * levels, width), jnp.float32)
    in_specs = [SMEM, HBM] + [HBM] * len(held)
    args = [region, weights, *held]
    out_shape = [
        jax.ShapeDtypeStruct((count * share, rows, width), jnp.float32),
        jax.ShapeDtypeStruct((chips * share, rows, width), jnp.float32),
    ]
    out_specs = [HBM, HBM]
    scratch = [whole, whole, pltpu.VMEM((share, members, members), jnp.float32)]
    scratch += [DMA((share,)), DMA((count,)), DMA((count,)), DMA((chips,))]
    if second:
        in_specs += [VMEM, HBM]
        args += [area, first]
        out_shape.append(jax.ShapeDtypeStruct((members, width), jnp.float32))
        out_specs.append(VMEM)
        scratch = [whole, DMA((count,))] + scratch
    return pl.pallas_call(
        functools.partial(mix_kernel, chips, share, levels, len(held), second),
        in_specs=in_specs,
        out_specs=out_specs,
        out_shape=out_shape,
        scratch_shapes=scratch,
        compiler_params=PARAMS,
        name="mix2" if second else "mix1",
    )(*args)


def join_kernel(chips, share, levels, scaled, size, *refs):
    if scaled:
        factor_ref, refs = refs[0], refs[1:]
    held, (out_ref, buf, sem_in, sem_out) = refs[:size], refs[size:]
    me = lax.axis_index("mem")
    loads, stores = [], []
    for i, (place, blocks) in enumerate(sources(me, chips, share, held)):
        loads.append(pltpu.make_async_copy(blocks, buf.at[i], sem_in.at[i]))
        spot = pl.ds(place * share, share)
        stores.append(pltpu.make_async_copy(buf.at[i], out_ref.at[spot], sem_out.at[i]))
    for copy in loads:
        copy.start()
    for i, (load, store) in enumerate(zip(loads, stores)):
        load.wait()
        if scaled:
            for member in range(buf.shape[2] // levels):
                spot = pl.ds(member * levels, levels)
                buf[i, :, spot, :] = buf[i, :, spot, :] * factor_ref[member]
        store.start()
    for copy in stores:
        copy.wait()


def join(held, chips, share, levels, factor=None):
    count = 2 * chips
    tail = held[0].shape[1:]
    scaled = factor is not None
    return pl.pallas_call(
        functools.partial(join_kernel, chips, share, levels, scaled, len(held)),
        in_specs=[SMEM] * scaled + [HBM] * len(held),
        out_specs=HBM,
        out_shape=jax.ShapeDtypeStruct((count * share, *tail), jnp.float32),
        scratch_shapes=[pltpu.VMEM((count, share, *tail), jnp.float32), DMA((count,)), DMA((count,))],
        compiler_params=PARAMS,
        name="join_scaled" if scaled else "join",
    )(*([factor] if scaled else []), *held)


def whole(dp_fore, hum_fore, area, region, weights, target):
    nblocks, mine, levels, width = dp_fore.shape
    groups = lax.axis_size("mem")
    chips = groups // 2
    share = nblocks // groups
    me = lax.axis_index("mem")
    count_all = nblocks * width * lax.axis_size("space") * levels
    swap_pairs = [(2 * z + c, 2 * z + 1 - c) for z in range(chips) for c in range(2)]

    def exchange(x, part):
        swapped = lax.ppermute(part, "mem", swap_pairs)
        pieces = pack(x, swapped, chips, share)
        sent = []
        for piece, d in zip(pieces, steps_of(chips)):
            pairs = [(2 * z + c, 2 * ((z + d) % chips) + c) for z in range(chips) for c in range(2)]
            sent.append(lax.ppermute(piece, "mem", pairs))
        return [x, swapped, *sent]

    dp = dp_fore.reshape(nblocks, mine * levels, width)
    hum = hum_fore.reshape(nblocks, mine * levels, width)
    own_area = lax.dynamic_slice_in_dim(area, me * share, share)

    dp_in = [lax.all_to_all(dp, "mem", 0, 0, tiled=True)]
    hum_in = exchange(hum, cut(hum, chips, share))
    dp_mixed, dp_cut = mix(region, weights, dp_in, chips, share, levels)
    dp_back = exchange(dp_mixed, dp_cut)
    hum_mixed, hum_cut, partial = mix(region, weights, hum_in, chips, share, levels, own_area, dp_mixed)
    parts = jnp.sum(partial, axis=1).reshape(groups, mine)
    local = lax.all_to_all(parts, "mem", 0, 0, tiled=True).sum(axis=0)
    spread = jnp.broadcast_to(local[None], (lax.axis_size("space"), mine))
    totals = lax.all_to_all(spread, "space", 0, 0, tiled=True).sum(axis=0)
    factor = target / (totals / count_all)
    hum_back = exchange(hum_mixed, hum_cut)
    dp_out = join(dp_back, chips, share, levels, factor)
    hum_out = join(hum_back, chips, share, levels)
    shape = (nblocks, mine, levels, width)
    return dp_out.reshape(shape), hum_out.reshape(shape)


def solution(mesh):
    return jax.shard_map(
        whole,
        mesh=mesh,
        in_specs=(
            P("space", "mem", None, None),
            P("space", "mem", None, None),
            P("space", None),
            P("space"),
            P(),
            P("mem"),
        ),
        out_specs=(P("space", "mem", None, None), P("space", "mem", None, None)),
        check_vma=False,
    )
```

```python
import functools

import jax
import jax.numpy as jnp
from jax import lax
from jax.experimental import pallas as pl
from jax.experimental.pallas import tpu as pltpu
from jax.sharding import PartitionSpec as P


HBM = pl.BlockSpec(memory_space=pltpu.HBM)
SMEM = pl.BlockSpec(memory_space=pltpu.SMEM)
VMEM = pl.BlockSpec(memory_space=pltpu.VMEM)
DMA = pltpu.SemaphoreType.DMA
PARAMS = pltpu.CompilerParams(vmem_limit_bytes=67_000_000)
ORDERS = {"dp_in": "middle", "hum_in": "middle", "dp_back": "mixed", "hum_back": "mixed"}
ROOMY = pltpu.CompilerParams(vmem_limit_bytes=32 * 1024 * 1024)


def steps_of(chips):
    half = chips // 2
    steps = [half]
    for d in range(half - 1, 0, -1):
        steps += [d, -d]
    return steps


def order_of(chips, name):
    steps = steps_of(chips)
    kind = ORDERS[name]
    if kind == "mixed":
        return steps[-2:] + steps[:-2]
    if kind == "middle":
        return steps[:1] + steps[-2:] + steps[1:-2]
    return steps


def device_at(me, chips, d, f):
    z, c = me // 2, me % 2
    return 2 * lax.rem(z + (d + chips), chips) + (c if f == 0 else 1 - c)


def sources(me, chips, share, refs, steps, at=0):
    own, swapped, *pieces = refs
    found = []
    if len(pieces) > len(steps):
        for f in (0, 1):
            found.append((device_at(me, chips, -steps[0], f), pieces[f].at[pl.ds(at, share)]))
        pieces, steps = pieces[2:], steps[1:]
    for piece, d in zip(pieces, steps):
        for f in (0, 1):
            found.append((device_at(me, chips, -d, f), piece.at[pl.ds(f * share, share)]))
    found.append((device_at(me, chips, 0, 1), swapped.at[pl.ds((me // 2) * share, share)]))
    found.append((me, own.at[pl.ds(me * share, share)]))
    return found


def run(copies):
    for copy in copies:
        copy.start()
    for copy in copies:
        copy.wait()


def relay(loads, stores):
    for copy in loads:
        copy.start()
    for load, store in zip(loads, stores):
        load.wait()
        store.start()
    for copy in stores:
        copy.wait()


def cut_kernel(chips, share, x_ref, out_ref, buf, sem_in, sem_out):
    flip = 1 - lax.axis_index("mem") % 2
    loads, stores = [], []
    for z in range(chips):
        spot = pl.ds((2 * z + flip) * share, share)
        loads.append(pltpu.make_async_copy(x_ref.at[spot], buf.at[z], sem_in.at[z]))
        stores.append(pltpu.make_async_copy(buf.at[z], out_ref.at[pl.ds(z * share, share)], sem_out.at[z]))
    relay(loads, stores)


def cut(x, chips, share):
    tail = x.shape[1:]
    return pl.pallas_call(
        functools.partial(cut_kernel, chips, share),
        in_specs=[HBM],
        out_specs=HBM,
        out_shape=jax.ShapeDtypeStruct((chips * share, *tail), x.dtype),
        scratch_shapes=[pltpu.VMEM((chips, share, *tail), x.dtype), DMA((chips,)), DMA((chips,))],
        compiler_params=PARAMS,
        name="cut",
    )(x)


def cut_far_kernel(chips, share, step, x_ref, y_ref, *refs):
    outs, (buf, sem_in, sem_out) = refs[:2], refs[2:]
    me = lax.axis_index("mem")
    loads, stores = [], []
    for f in (0, 1):
        spot = pl.ds(device_at(me, chips, step, f) * share, share)
        for i, ref in enumerate((x_ref, y_ref)):
            half = pl.ds(i * share, share)
            loads.append(pltpu.make_async_copy(ref.at[spot], buf.at[f, half], sem_in.at[2 * f + i]))
            stores.append(pltpu.make_async_copy(buf.at[f, half], outs[f].at[half], sem_out.at[2 * f + i]))
    relay(loads, stores)


def cut_far(x, y, chips, share, step):
    piece = (2 * share, *x.shape[1:])
    return pl.pallas_call(
        functools.partial(cut_far_kernel, chips, share, step),
        in_specs=[HBM, HBM],
        out_specs=[HBM] * 2,
        out_shape=[jax.ShapeDtypeStruct(piece, x.dtype)] * 2,
        scratch_shapes=[pltpu.VMEM((2, *piece), x.dtype), DMA((4,)), DMA((4,))],
        compiler_params=PARAMS,
        name="cut_far",
    )(x, y)


def pack_kernel(chips, share, steps, x_ref, swapped_ref, *refs):
    count = len(steps)
    outs, (buf, sem_in, sem_other, sem_out) = refs[:count], refs[count:]
    me = lax.axis_index("mem")
    loads, others, stores = [], [], []
    for i, d in enumerate(steps):
        to = device_at(me, chips, d, 0)
        own, rest = pl.ds(to * share, share), pl.ds((to // 2) * share, share)
        loads.append(pltpu.make_async_copy(x_ref.at[own], buf.at[i, pl.ds(0, share)], sem_in.at[i]))
        others.append(
            pltpu.make_async_copy(swapped_ref.at[rest], buf.at[i, pl.ds(share, share)], sem_other.at[i])
        )
        stores.append(pltpu.make_async_copy(buf.at[i], outs[i], sem_out.at[i]))
    for load, rest in zip(loads, others):
        load.start()
        rest.start()
    for load, rest, store in zip(loads, others, stores):
        load.wait()
        rest.wait()
        store.start()
    for copy in stores:
        copy.wait()


def pack(x, swapped, chips, share, steps):
    piece = (2 * share, *x.shape[1:])
    count = len(steps)
    return pl.pallas_call(
        functools.partial(pack_kernel, chips, share, steps),
        in_specs=[HBM, HBM],
        out_specs=[HBM] * count,
        out_shape=[jax.ShapeDtypeStruct(piece, x.dtype)] * count,
        scratch_shapes=[pltpu.VMEM((count, *piece), x.dtype), DMA((count,)), DMA((count,)), DMA((count,))],
        compiler_params=PARAMS,
        name="pack",
    )(x, swapped)


def mix_kernel(chips, share, levels, steps, size, second, *refs):
    count = 2 * chips
    region_ref, weights_ref = refs[:2]
    held, refs = refs[2 : 2 + size], refs[2 + size :]
    if second:
        area_ref, first_ref, *refs = refs
    out_ref, cut_ref, *refs = refs
    if second:
        mass_ref, f_buf, sem_f, *refs = refs
    x_buf, y_buf, w_buf, sem_w, sem_in, sem_out, sem_cut = refs
    me = lax.axis_index("mem")
    flip = 1 - me % 2
    rows = out_ref.shape[1]
    width = out_ref.shape[2]
    members = w_buf.shape[1]

    def lines(place):
        return pl.ds(place * rows if isinstance(place, int) else pl.multiple_of(place * rows, rows), rows)

    copies = []
    for b in range(share):
        table = region_ref[me * share + b]
        copies.append(pltpu.make_async_copy(weights_ref.at[table], w_buf.at[b], sem_w.at[b]))
    for i, (place, blocks) in enumerate(sources(me, chips, share, held, steps, share if second else 0)):
        copies.append(pltpu.make_async_copy(blocks, x_buf.at[:, lines(place)], sem_in.at[i]))
    if second:
        for place in range(count):
            blocks = first_ref.at[pl.ds(place * share, share)]
            copies.append(pltpu.make_async_copy(blocks, f_buf.at[:, lines(place)], sem_f.at[place]))
    run(copies)

    step = 4
    if second:
        total = jnp.zeros((members, width), jnp.float32)
    for b in range(share):
        table = w_buf[b]
        for first in range(0, levels, step):
            x = jnp.concatenate(
                [x_buf[b, pl.ds(first + l, members, stride=levels), :] for l in range(step)], axis=1
            )
            y = lax.dot_general(
                table,
                x,
                (((0,), (0,)), ((), ())),
                precision=lax.Precision.HIGHEST,
                preferred_element_type=jnp.float32,
            )
            for l in range(step):
                part = y[:, l * width : (l + 1) * width]
                y_buf[b, pl.ds(first + l, members, stride=levels), :] = part
                if second:
                    mixed = f_buf[b, pl.ds(first + l, members, stride=levels), :]
                    total += area_ref[b] * mixed * (1.0 - part)
    if second:
        mass_ref[...] = total

    copies = []
    for z in range(chips):
        spot = pl.ds(z * share, share)
        copies.append(pltpu.make_async_copy(y_buf.at[:, lines(2 * z + flip)], cut_ref.at[spot], sem_cut.at[z]))
    for place in range(count):
        spot = pl.ds(place * share, share)
        copies.append(pltpu.make_async_copy(y_buf.at[:, lines(place)], out_ref.at[spot], sem_out.at[place]))
    run(copies)


def mix(region, weights, held, chips, share, levels, steps, area=None, first=None):
    second = area is not None
    rows, width = held[0].shape[1:]
    members = weights.shape[1]
    count = 2 * chips
    whole = pltpu.VMEM((share, members * levels, width), jnp.float32)
    in_specs = [SMEM, HBM] + [HBM] * len(held)
    args = [region, weights, *held]
    out_shape = [
        jax.ShapeDtypeStruct((count * share, rows, width), jnp.float32),
        jax.ShapeDtypeStruct((chips * share, rows, width), jnp.float32),
    ]
    out_specs = [HBM, HBM]
    scratch = [whole, whole, pltpu.VMEM((share, members, members), jnp.float32)]
    scratch += [DMA((share,)), DMA((count,)), DMA((count,)), DMA((chips,))]
    if second:
        in_specs += [VMEM, HBM]
        args += [area, first]
        out_shape.append(jax.ShapeDtypeStruct((members, width), jnp.float32))
        out_specs.append(VMEM)
        scratch = [whole, DMA((count,))] + scratch
    return pl.pallas_call(
        functools.partial(mix_kernel, chips, share, levels, steps, len(held), second),
        in_specs=in_specs,
        out_specs=out_specs,
        out_shape=out_shape,
        scratch_shapes=scratch,
        compiler_params=PARAMS,
        name="mix2" if second else "mix1",
    )(*args)


def join_kernel(chips, share, levels, steps, scaled, size, picked, *refs):
    if scaled:
        factor_ref, refs = refs[0], refs[1:]
    held, (out_ref, buf, sem_in, sem_out) = refs[:size], refs[size:]
    me = lax.axis_index("mem")
    loads, stores = [], []
    for i, (place, blocks) in enumerate(sources(me, chips, share, held, steps)[j] for j in picked):
        loads.append(pltpu.make_async_copy(blocks, buf.at[i], sem_in.at[i]))
        spot = pl.ds(place * share, share)
        stores.append(pltpu.make_async_copy(buf.at[i], out_ref.at[spot], sem_out.at[i]))
    for copy in loads:
        copy.start()
    for i, (load, store) in enumerate(zip(loads, stores)):
        load.wait()
        if scaled:
            for member in range(buf.shape[2] // levels):
                spot = pl.ds(member * levels, levels)
                buf[i, :, spot, :] = buf[i, :, spot, :] * factor_ref[member]
        store.start()
    for copy in stores:
        copy.wait()


def join(held, chips, share, levels, steps, factor=None, late=0):
    count = 2 * chips
    tail = held[0].shape[1:]
    scaled = factor is not None
    picked = [i for i in range(count) if not count - 2 - 2 * late <= i < count - 2]
    held = held[: len(held) - late] + held[-1 - late : len(held) - late] * late
    return pl.pallas_call(
        functools.partial(join_kernel, chips, share, levels, steps, scaled, len(held), picked),
        in_specs=[SMEM] * scaled + [HBM] * len(held),
        out_specs=HBM,
        out_shape=jax.ShapeDtypeStruct((count * share, *tail), jnp.float32),
        scratch_shapes=[pltpu.VMEM((len(picked), share, *tail), jnp.float32), DMA((count,)), DMA((count,))],
        compiler_params=ROOMY,
        name="join_scaled" if scaled else "join_early",
    )(*([factor] if scaled else []), *held)


def join_late_kernel(chips, share, steps, *refs):
    pieces, (_, out_ref, sem) = refs[: len(steps)], refs[len(steps) :]
    me = lax.axis_index("mem")
    copies = []
    for i, (piece, d) in enumerate(zip(pieces, steps)):
        for f in (0, 1):
            spot = pl.ds(device_at(me, chips, -d, f) * share, share)
            blocks = piece.at[pl.ds(f * share, share)]
            copies.append(pltpu.make_async_copy(blocks, out_ref.at[spot], sem.at[2 * i + f]))
    run(copies)


def join_late(pieces, onto, chips, share, steps):
    count = len(pieces)
    pieces = [pltpu.with_memory_space_constraint(piece, pltpu.VMEM) for piece in pieces]
    return pl.pallas_call(
        functools.partial(join_late_kernel, chips, share, steps[-count:]),
        in_specs=[VMEM] * count + [HBM],
        out_specs=HBM,
        out_shape=jax.ShapeDtypeStruct(onto.shape, onto.dtype),
        scratch_shapes=[DMA((2 * count,))],
        input_output_aliases={count: 0},
        compiler_params=ROOMY,
        name="join_late",
    )(*pieces, onto)


def whole(dp_fore, hum_fore, area, region, weights, target):
    nblocks, mine, levels, width = dp_fore.shape
    groups = lax.axis_size("mem")
    chips = groups // 2
    share = nblocks // groups
    me = lax.axis_index("mem")
    count_all = nblocks * width * lax.axis_size("space") * levels

    def along(piece, d, f=0):
        pairs = [(2 * z + c, 2 * ((z + d) % chips) + (c ^ f)) for z in range(chips) for c in range(2)]
        return lax.ppermute(piece, "mem", pairs)

    def exchange(x, part, name, far=()):
        steps = order_of(chips, name)
        sent = [*far]
        if far:
            steps = steps[1:]
        if part is None:
            part = cut(x, chips, share)
        swapped = along(part, 0, 1)
        pieces = pack(x, swapped, chips, share, steps)
        for piece, d in zip(pieces, steps):
            sent.append(along(piece, d))
        return [x, swapped, *sent]

    dp = dp_fore.reshape(nblocks, mine * levels, width)
    hum = hum_fore.reshape(nblocks, mine * levels, width)
    own_area = lax.dynamic_slice_in_dim(area, me * share, share)

    half = chips // 2
    far = [along(piece, half, f) for f, piece in enumerate(cut_far(dp, hum, chips, share, half))]
    dp_in = exchange(dp, None, "dp_in", far)
    hum_in = exchange(hum, None, "hum_in", far)
    dp_mixed, dp_cut = mix(region, weights, dp_in, chips, share, levels, order_of(chips, "dp_in"))
    dp_back = exchange(dp_mixed, dp_cut, "dp_back")
    hum_mixed, hum_cut, partial = mix(region, weights, hum_in, chips, share, levels, order_of(chips, "hum_in"), own_area, dp_mixed)
    parts = jnp.sum(partial, axis=1).reshape(groups, mine)
    local = lax.all_to_all(parts, "mem", 0, 0, tiled=True).sum(axis=0)
    spread = jnp.broadcast_to(local[None], (lax.axis_size("space"), mine))
    totals = lax.all_to_all(spread, "space", 0, 0, tiled=True).sum(axis=0)
    factor = target / (totals / count_all)
    hum_back = exchange(hum_mixed, hum_cut, "hum_back")
    dp_out = join(dp_back, chips, share, levels, order_of(chips, "dp_back"), factor)
    late = 4
    last = order_of(chips, "hum_back")
    hum_early = join(hum_back, chips, share, levels, last, late=late)
    hum_out = join_late(hum_back[-late:], hum_early, chips, share, last)
    shape = (nblocks, mine, levels, width)
    return dp_out.reshape(shape), hum_out.reshape(shape)


def solution(mesh):
    return jax.shard_map(
        whole,
        mesh=mesh,
        in_specs=(
            P("space", "mem", None, None),
            P("space", "mem", None, None),
            P("space", None),
            P("space"),
            P(),
            P("mem"),
        ),
        out_specs=(P("space", "mem", None, None), P("space", "mem", None, None)),
        check_vma=False,
    )
```
